16 devices in a mesh: dp: 2 (over y, z), ep: 8 (over x, core).
Axes of the slice: x: 4, y: 2, z: 1, core: 2. Of those that a mesh axis runs over, the one named last changes fastest.
The devices are a block of a 4x4x8 slice.
Arguments:
- x: bfloat16 [16384, 2048], P(('dp', 'ep')), parts along dimension 0
- route_idx: int32 [16384, 4], P(('dp', 'ep')), parts along dimension 0
- route_gate: float32 [16384, 4], P(('dp', 'ep')), parts along dimension 0
- w_gate: bfloat16 [8, 2048, 1408], P('ep')
- w_up: bfloat16 [8, 2048, 1408], P('ep')
- w_down: bfloat16 [8, 1408, 2048], P('ep')
- grad_y: bfloat16 [16384, 2048], P(('dp', 'ep')), parts along dimension 0
Outputs:
- output 1: bfloat16 [16384, 2048], P(('dp', 'ep')), parts along dimension 0
- output 2: bfloat16 [16384, 2048], P(('dp', 'ep')), parts along dimension 0
- output 3: bfloat16 [16, 2048, 1408], P(('dp', 'ep')), parts along dimension 0
- output 4: bfloat16 [16, 2048, 1408], P(('dp', 'ep')), parts along dimension 0
- output 5: bfloat16 [16, 1408, 2048], P(('dp', 'ep')), parts along dimension 0
There are 2 independent parts. The reference program is written for one: setup_inputs(seed, part) draws one part's arguments, and reference() takes and returns one part's arrays. A program takes and returns all parts, laid end to end along the dimension named above; an argument that names none is the same for every part.
All inputs are finite; a program needn't handle non-finite values.
Results may differ from the reference program's by a relative error of at most 0.00155.
Values are sent between devices in bfloat16 or wider.
A program may use at most 768 MiB of HBM per device.

```python
import jax
import jax.numpy as jnp
from jax import lax

GROUP_SIZE = 8
TOKENS = 1024
D_MODEL = 2048
D_FF = 1408
TOP_K = 4
ROW_BLOCK = 64
CAPACITY = 3 * TOKENS // 4
T_ALL = GROUP_SIZE * TOKENS


def draw_routes(route_key):
    order_key, src_key = jax.random.split(route_key)
    expert_order = jax.random.permutation(order_key, GROUP_SIZE).astype(jnp.int32)
    hot_count = TOP_K // 2
    cold_count = GROUP_SIZE - hot_count
    spare = TOP_K * TOKENS - hot_count * CAPACITY - cold_count
    slot_ids = jnp.arange(TOP_K * TOKENS, dtype=jnp.int32)

    def one_source(one_key):
        unit_key, row_key = jax.random.split(one_key)
        units = jax.random.permutation(unit_key, cold_count * (CAPACITY - 1))[:spare] // (CAPACITY - 1)
        cold_load = 1 + jnp.bincount(units, length=cold_count)
        loads = jnp.concatenate([jnp.full((hot_count,), CAPACITY, jnp.int32), cold_load.astype(jnp.int32)])
        run_ends = jnp.cumsum(loads)
        run_index = jnp.searchsorted(run_ends, slot_ids, side="right")
        grid = expert_order[run_index].reshape(TOP_K, TOKENS).T
        return grid[jax.random.permutation(row_key, TOKENS)]

    return jax.vmap(one_source)(jax.random.split(src_key, GROUP_SIZE)).reshape(T_ALL, TOP_K)


def setup_inputs(seed: int = 0, part: int = 0) -> dict:
    part_key = jax.random.fold_in(jax.random.key(seed), part)
    x_key, gate_key, grad_key, route_key = jax.random.split(part_key, 4)
    wg_key, wu_key, wd_key = jax.random.split(jax.random.key(seed + 1), 3)
    x = jax.random.normal(x_key, (T_ALL, D_MODEL), jnp.float32).astype(jnp.bfloat16)
    route_gate = jax.random.uniform(gate_key, (T_ALL, TOP_K), jnp.float32, 0.3, 0.7)
    grad_y = jax.random.normal(grad_key, (T_ALL, D_MODEL), jnp.float32).astype(jnp.bfloat16)
    w_gate = (jax.random.normal(wg_key, (GROUP_SIZE, D_MODEL, D_FF), jnp.float32) * D_MODEL ** -0.5).astype(jnp.bfloat16)
    w_up = (jax.random.normal(wu_key, (GROUP_SIZE, D_MODEL, D_FF), jnp.float32) * D_MODEL ** -0.5).astype(jnp.bfloat16)
    w_down = (jax.random.normal(wd_key, (GROUP_SIZE, D_FF, D_MODEL), jnp.float32) * D_FF ** -0.5).astype(jnp.bfloat16)
    return {"x": x, "route_idx": draw_routes(route_key), "route_gate": route_gate, "w_gate": w_gate, "w_up": w_up, "w_down": w_down, "grad_y": grad_y}


def expert_block(rows, out_cot, gate_mat, up_mat, down_mat):
    pre_gate = jnp.dot(rows, gate_mat, preferred_element_type=jnp.float32)
    pre_up = jnp.dot(rows, up_mat, preferred_element_type=jnp.float32)
    sig_gate = jax.nn.sigmoid(pre_gate)
    hidden = (pre_gate * sig_gate * pre_up).astype(jnp.bfloat16)
    expert_out = jnp.dot(hidden, down_mat, preferred_element_type=jnp.float32).astype(jnp.bfloat16)
    grad_hidden = jnp.dot(out_cot, down_mat.T, preferred_element_type=jnp.float32).astype(jnp.bfloat16).astype(jnp.float32)
    grad_gate = (grad_hidden * pre_up * (sig_gate * (1.0 + pre_gate * (1.0 - sig_gate)))).astype(jnp.bfloat16)
    grad_up = (grad_hidden * (pre_gate * sig_gate)).astype(jnp.bfloat16)
    grad_rows = (jnp.dot(grad_gate, gate_mat.T, preferred_element_type=jnp.float32) + jnp.dot(grad_up, up_mat.T, preferred_element_type=jnp.float32)).astype(jnp.bfloat16)
    grad_gate_mat = jnp.dot(rows.T, grad_gate, preferred_element_type=jnp.float32)
    grad_up_mat = jnp.dot(rows.T, grad_up, preferred_element_type=jnp.float32)
    grad_down_mat = jnp.dot(hidden.T, out_cot, preferred_element_type=jnp.float32)
    return expert_out, grad_rows, grad_gate_mat, grad_up_mat, grad_down_mat


def reference(x, route_idx, route_gate, w_gate, w_up, w_down, grad_y):
    n_slots = T_ALL * TOP_K
    n_blocks = n_slots // ROW_BLOCK + GROUP_SIZE
    flat_exp = route_idx.reshape(n_slots)
    order = jnp.argsort(flat_exp, stable=True).astype(jnp.int32)
    sorted_exp = flat_exp[order]
    exp_counts = jnp.bincount(flat_exp, length=GROUP_SIZE).astype(jnp.int32)
    exp_starts = jnp.cumsum(exp_counts) - exp_counts
    padded = (exp_counts + ROW_BLOCK - 1) // ROW_BLOCK * ROW_BLOCK
    pad_ends = jnp.cumsum(padded)
    dest_pos = pad_ends[sorted_exp] - padded[sorted_exp] + jnp.arange(n_slots, dtype=jnp.int32) - exp_starts[sorted_exp]
    slot_at = jnp.full((n_blocks * ROW_BLOCK,), n_slots, jnp.int32).at[dest_pos].set(order)
    filled = slot_at < n_slots
    safe_slot = jnp.where(filled, slot_at, 0)
    tok_at = safe_slot // TOP_K
    gate_at = jnp.where(filled, route_gate.reshape(n_slots)[safe_slot], 0.0)
    rows = jnp.where(filled[:, None], x[tok_at], 0)
    out_cot = (gate_at[:, None] * grad_y[tok_at].astype(jnp.float32)).astype(jnp.bfloat16)
    block_exp = jnp.minimum(jnp.searchsorted(pad_ends, jnp.arange(n_blocks, dtype=jnp.int32) * ROW_BLOCK, side="right"), GROUP_SIZE - 1)

    def block_step(carry, item):
        acc_gate, acc_up, acc_down = carry
        expert, blk_rows, blk_cot = item
        blk_out, blk_grad, gate_part, up_part, down_part = expert_block(blk_rows, blk_cot, w_gate[expert], w_up[expert], w_down[expert])
        carry = (acc_gate.at[expert].add(gate_part), acc_up.at[expert].add(up_part), acc_down.at[expert].add(down_part))
        return carry, (blk_out, blk_grad)

    init = (jnp.zeros((GROUP_SIZE, D_MODEL, D_FF), jnp.float32), jnp.zeros((GROUP_SIZE, D_MODEL, D_FF), jnp.float32), jnp.zeros((GROUP_SIZE, D_FF, D_MODEL), jnp.float32))
    blocks_in = (block_exp, rows.reshape(n_blocks, ROW_BLOCK, D_MODEL), out_cot.reshape(n_blocks, ROW_BLOCK, D_MODEL))
    (acc_gate, acc_up, acc_down), (outs, grads) = lax.scan(block_step, init, blocks_in)
    outs = outs.reshape(n_blocks * ROW_BLOCK, D_MODEL)
    grads = grads.reshape(n_blocks * ROW_BLOCK, D_MODEL)
    y = jax.ops.segment_sum(gate_at[:, None] * outs.astype(jnp.float32), tok_at, num_segments=T_ALL)
    grad_x = jax.ops.segment_sum(grads.astype(jnp.float32), tok_at, num_segments=T_ALL)
    return (y.astype(jnp.bfloat16), grad_x.astype(jnp.bfloat16), acc_gate.astype(jnp.bfloat16), acc_up.astype(jnp.bfloat16), acc_down.astype(jnp.bfloat16))
```

```python
import functools

import jax
import jax.numpy as jnp
from jax import lax
from jax.experimental import pallas as pl
from jax.experimental.pallas import tpu as pltpu
from jax.sharding import PartitionSpec as P

MESH = pl.DeviceIdType.MESH
MID = (((1,), (0,)), ((), ()))
LAST = (((1,), (1,)), ((), ()))
FIRST = (((0,), (0,)), ((), ()))
BF = jnp.bfloat16
F32 = jnp.float32


def dot(a, b, dims=MID):
    return lax.dot_general(a, b, dims, preferred_element_type=F32)


def layer_kernel(n, cap, x_ref, gy_ref, meta_ref, wg_ref, wu_ref, wd_ref,
                 xr_out, a_out, b_out, h_out, o_out, c_out, da_out, db_out, r_out, back_o, xg, gyg, mg,
                 wg, wu, wd, xbuf, mbuf, tri, pbuf, posbuf, xr, ab_a, ab_b, hb, ob, cb, dab, dbb,
                 send_sem, recv_sem, osend_sem, orecv_sem, wsem, lsem, outsem):
    tok, d = x_ref.shape
    ff = wd_ref.shape[1]
    half = tok // 2
    me = lax.axis_index("ep")
    chips = n // 2
    chip, core = me // 2, lax.rem(me, 2)
    right = lax.rem(chip + 1, chips) * 2 + core
    left = lax.rem(chip + chips - 1, chips) * 2 + core
    across = lax.rem(chip + 2, chips) * 2 + core
    mate = chip * 2 + 1 - core
    right_m = lax.rem(chip + 1, chips) * 2 + 1 - core
    left_m = lax.rem(chip + chips - 1, chips) * 2 + 1 - core
    across_m = lax.rem(chip + 2, chips) * 2 + 1 - core
    order = (me, mate, left, right, left_m, right_m, across, across_m)

    barrier = pltpu.get_barrier_semaphore()
    for peer in order[1:]:
        pl.semaphore_signal(barrier, inc=1, device_id={"ep": peer}, device_id_type=MESH)
    pl.semaphore_wait(barrier, n - 1)

    own = (x_ref, gy_ref, meta_ref)
    got = (xg, gyg, mg)

    def part(item, slot, which):
        if item == 2 or which is None:
            return got[item].at[slot]
        return got[item].at[slot, pl.ds(which * half, half)]

    def send(item, k):
        src, dst, peer = {
            0: (own[item], part(item, me, None), right),
            1: (own[item], part(item, me, None), left),
            2: (own[item], part(item, me, None), mate),
            3: (part(item, left, 0), part(item, left, 0), right),
            4: (part(item, right, 1), part(item, right, 1), left),
            5: (part(item, left, None), part(item, left, None), mate),
            6: (part(item, right, None), part(item, right, None), mate),
            7: (part(item, across, None), part(item, across, None), mate),
        }[k]
        return pltpu.make_async_remote_copy(
            src_ref=src, dst_ref=dst, send_sem=send_sem.at[item, k], recv_sem=recv_sem.at[item, k],
            device_id={"ep": peer}, device_id_type=MESH)

    def land(item, k):
        ref = {
            0: part(item, left, None), 1: part(item, right, None), 2: part(item, mate, None),
            3: part(item, across, 0), 4: part(item, across, 1),
            5: part(item, left_m, None), 6: part(item, right_m, None), 7: part(item, across_m, None),
        }[k]
        pltpu.make_async_remote_copy(
            src_ref=ref, dst_ref=ref, send_sem=send_sem.at[item, k], recv_sem=recv_sem.at[item, k],
            device_id={"ep": mate}, device_id_type=MESH).wait_recv()

    def give(j):
        to = order[j]
        return pltpu.make_async_remote_copy(
            src_ref=o_out.at[rows_of(to)], dst_ref=back_o.at[rows_of(me)], send_sem=osend_sem.at[j], recv_sem=orecv_sem.at[me],
            device_id={"ep": to}, device_id_type=MESH)

    def taken(j):
        ref = back_o.at[rows_of(order[j])]
        pltpu.make_async_remote_copy(
            src_ref=ref, dst_ref=ref, send_sem=osend_sem.at[j], recv_sem=orecv_sem.at[order[j]],
            device_id={"ep": mate}, device_id_type=MESH).wait_recv()

    for k in (0, 1, 2):
        send(2, k).start()
    for k in (0, 1, 2):
        send(0, k).start()
    send(1, 2).start()

    weights = [pltpu.make_async_copy(s.at[0], t, wsem.at[q]) for q, (s, t) in enumerate(((wg_ref, wg), (wu_ref, wu), (wd_ref, wd)))]
    for cp in weights:
        cp.start()
    for q in range(4):
        rows = lax.broadcasted_iota(jnp.int32, (tok // 4, tok), 0) + q * (tok // 4)
        cols = lax.broadcasted_iota(jnp.int32, (tok // 4, tok), 1)
        tri[pl.ds(q * (tok // 4), tok // 4), :] = jnp.where(rows <= cols, 1.0, 0.0).astype(BF)
    for cp in weights:
        cp.wait()

    def is_forward(i):
        return (i < 2) | ((i >= 4) & (i < 10))

    def slot_of(i):
        j = jnp.where(i < 2, i, jnp.where(i < 10, i - 2, i - 8))
        hop = jnp.where(j < 2, 0, jnp.where(j >= 6, 2, jnp.where(lax.rem(j, 2) == 0, chips - 1, 1)))
        flip = (j == 1) | (j == 4) | (j == 5) | (j == 7)
        return j, lax.rem(chip + hop, chips) * 2 + jnp.where(flip, 1 - core, core)

    def rows_of(slot):
        return pl.ds(pl.multiple_of(slot * cap, cap), cap)

    f_bufs = ((xr, xr_out), (ab_a, a_out), (ab_b, b_out), (hb, h_out), (ob, o_out))
    b_bufs = ((cb, c_out), (dab, da_out), (dbb, db_out), (ob, r_out))

    def out_copy(q, bufs, slot):
        src, dst = bufs[q]
        return pltpu.make_async_copy(src, dst.at[rows_of(slot)], outsem.at[q + (5 if bufs is b_bufs else 0)])

    def col_tiles(body):
        wide = ff // 256

        def run(t, c):
            body(pl.ds(pl.multiple_of(t * 256, 256), 256))
            return c

        lax.fori_loop(0, wide, run, 0)
        if ff % 256:
            body(pl.ds(wide * 256, ff % 256))

    def model_tiles(body):
        def run(t, c):
            body(pl.ds(pl.multiple_of(t * 512, 512), 512))
            return c

        lax.fori_loop(0, d // 512, run, 0)

    def settle(i):
        last = i - 1

        @pl.when((i > 0) & is_forward(last))
        def _():
            for q in range(5):
                out_copy(q, f_bufs, 0).wait()

        @pl.when((i > 0) & jnp.logical_not(is_forward(last)))
        def _():
            for q in range(4):
                out_copy(q, b_bufs, 0).wait()

        for when, js in ((2, (1,)), (9, (2, 3, 4, 5, 6)), (10, (7,))):
            @pl.when(i == when)
            def _(js=js):
                for j in js:
                    give(j).start()

    def step(i, carry):
        is_f = is_forward(i)
        j, slot = slot_of(i)

        @pl.when(i == 1)
        def _():
            land(0, 2)
            land(2, 2)

        @pl.when(i == 3)
        def _():
            land(1, 2)

        @pl.when(i == 4)
        def _():
            for k in (0, 1):
                land(2, k)
                land(0, k)
            for k in (3, 5, 6):
                send(2, k).start()
            for k in (3, 4, 5, 6):
                send(0, k).start()
            for k in (0, 1):
                send(1, k).start()

        @pl.when(i == 6)
        def _():
            for k in (5, 6):
                land(0, k)
                land(2, k)

        @pl.when(i == 8)
        def _():
            land(2, 3)
            land(0, 3)
            land(0, 4)
            send(2, 7).start()
            send(0, 7).start()

        @pl.when(i == 9)
        def _():
            land(2, 7)
            land(0, 7)
            land(1, 0)
            land(1, 1)
            for k in (3, 4, 5, 6):
                send(1, k).start()

        @pl.when(i == 12)
        def _():
            land(1, 5)
            land(1, 6)

        @pl.when(i == 14)
        def _():
            land(1, 3)
            land(1, 4)
            send(1, 7).start()

        @pl.when(i == 15)
        def _():
            land(1, 7)

        def fetch(own_ref, got_ref, buf, sem):
            @pl.when(j == 0)
            def _():
                pltpu.make_async_copy(own_ref, buf, sem).start()

            @pl.when(j > 0)
            def _():
                pltpu.make_async_copy(got_ref.at[slot], buf, sem).start()

        def fetched(own_ref, buf, sem):
            pltpu.make_async_copy(own_ref, buf, sem).wait()

        fetch(meta_ref, mg, mbuf, lsem.at[1])
        fetched(meta_ref, mbuf, lsem.at[1])
        sel = mbuf[0:4, :] == me.astype(F32)
        gate = jnp.sum(jnp.where(sel, mbuf[4:8, :], 0.0), axis=0, keepdims=True)

        def fill_p():
            pos = posbuf[j][0:1, :]
            for q in range(cap // 128):
                rows = lax.broadcasted_iota(jnp.int32, (128, tok), 0) + q * 128
                pbuf[pl.ds(q * 128, 128), :] = jnp.where(rows == pos, 1.0, 0.0).astype(BF)

        @pl.when(is_f)
        def _():
            fetch(x_ref, xg, xbuf, lsem.at[0])
            hit = jnp.max(jnp.where(sel, 1.0, 0.0), axis=0, keepdims=True)
            count = dot(jnp.broadcast_to(hit, (16, tok)).astype(BF), tri[...])[0:1, :]
            pos = jnp.where(hit > 0.0, count - 1.0, -1.0).astype(jnp.int32)
            posbuf[j] = jnp.broadcast_to(pos, (8, tok))
            fill_p()
            settle(i)
            fetched(x_ref, xbuf, lsem.at[0])

            def pick(cols):
                xr[:, cols] = dot(pbuf[...], xbuf[:, cols]).astype(BF)

            model_tiles(pick)
            out_copy(0, f_bufs, slot).start()

            def up(cols):
                a, b = dot(xr[...], wg[:, cols]), dot(xr[...], wu[:, cols])
                ab_a[:, cols] = a
                ab_b[:, cols] = b
                hb[:, cols] = (a * jax.nn.sigmoid(a) * b).astype(BF)

            col_tiles(up)
            for q in (1, 2, 3):
                out_copy(q, f_bufs, slot).start()

            def down(cols):
                ob[:, cols] = dot(hb[...], wd[:, cols]).astype(BF)

            model_tiles(down)

            @pl.when(j == 0)
            def _():
                pltpu.make_async_copy(ob, back_o.at[rows_of(me)], outsem.at[4]).start()

            @pl.when(j > 0)
            def _():
                out_copy(4, f_bufs, slot).start()

        @pl.when(jnp.logical_not(is_f))
        def _():
            fetch(gy_ref, gyg, xbuf, lsem.at[0])
            fill_p()
            settle(i)
            load_a = pltpu.make_async_copy(a_out.at[rows_of(slot)], ab_a, lsem.at[2])
            load_b = pltpu.make_async_copy(b_out.at[rows_of(slot)], ab_b, lsem.at[3])
            load_a.start()
            load_b.start()
            g = jnp.sum(pbuf[...].astype(F32) * gate, axis=1, keepdims=True)
            fetched(gy_ref, xbuf, lsem.at[0])

            def pick(cols):
                cb[:, cols] = (g * dot(pbuf[...], xbuf[:, cols])).astype(BF)

            model_tiles(pick)
            out_copy(0, b_bufs, slot).start()
            load_a.wait()
            load_b.wait()

            def down_t(cols):
                dh = dot(cb[...], wd[cols, :], LAST).astype(BF).astype(F32)
                a, b = ab_a[:, cols], ab_b[:, cols]
                s = jax.nn.sigmoid(a)
                dab[:, cols] = (dh * b * (s * (1.0 + a * (1.0 - s)))).astype(BF)
                dbb[:, cols] = (dh * (a * s)).astype(BF)

            col_tiles(down_t)
            out_copy(1, b_bufs, slot).start()
            out_copy(2, b_bufs, slot).start()

            def up_t(cols):
                ob[:, cols] = (dot(dab[...], wg[cols, :], LAST) + dot(dbb[...], wu[cols, :], LAST)).astype(BF)

            model_tiles(up_t)
            out_copy(3, b_bufs, slot).start()

        return carry

    lax.fori_loop(0, 2 * n, step, 0)
    settle(2 * n)
    for j in range(1, n):
        taken(j)
        give(j).wait_send()
    for item in range(3):
        for k in range(8):
            if (item, k) != (2, 4):
                send(item, k).wait_send()


def layer(n, cap, x, gy, meta, w_gate, w_up, w_down):
    tok, d = x.shape
    ff = w_down.shape[1]
    rows = n * cap
    hbm = pl.BlockSpec(memory_space=pltpu.HBM)
    shapes = [
        ((rows, d), BF), ((rows, ff), F32), ((rows, ff), F32), ((rows, ff), BF), ((rows, d), BF), ((rows, d), BF),
        ((rows, ff), BF), ((rows, ff), BF), ((rows, d), BF), ((rows, d), BF),
        ((n, tok, d), BF), ((n, tok, d), BF), ((n, 8, tok), F32)]
    dma = pltpu.SemaphoreType.DMA
    return pl.pallas_call(
        functools.partial(layer_kernel, n, cap),
        out_shape=[jax.ShapeDtypeStruct(s, t) for s, t in shapes],
        in_specs=[hbm] * 6,
        out_specs=[hbm] * len(shapes),
        scratch_shapes=[
            pltpu.VMEM((d, ff), BF),
            pltpu.VMEM((d, ff), BF),
            pltpu.VMEM((ff, d), BF),
            pltpu.VMEM((tok, d), BF),
            pltpu.VMEM((8, tok), F32),
            pltpu.VMEM((tok, tok), BF),
            pltpu.VMEM((cap, tok), BF),
            pltpu.VMEM((n, 8, tok), jnp.int32),
            pltpu.VMEM((cap, d), BF),
            pltpu.VMEM((cap, ff), F32),
            pltpu.VMEM((cap, ff), F32),
            pltpu.VMEM((cap, ff), BF),
            pltpu.VMEM((cap, d), BF),
            pltpu.VMEM((cap, d), BF),
            pltpu.VMEM((cap, ff), BF),
            pltpu.VMEM((cap, ff), BF),
            dma((3, 8)), dma((3, 8)), dma((n,)), dma((n,)), dma((3,)), dma((4,)), dma((9,)),
        ],
        compiler_params=pltpu.CompilerParams(collective_id=0, has_side_effects=True, vmem_limit_bytes=62 * 1024 * 1024),
        cost_estimate=pl.CostEstimate(flops=2 * rows * d * (6 * ff + 2 * tok), bytes_accessed=700 * 1024 * 1024, transcendentals=2 * rows * ff),
        name="layer",
    )(x, gy, meta, w_gate, w_up, w_down)


def combine_kernel(n, back_ref, pos_ref, gate_ref, out_ref, acc):
    e = pl.program_id(0)
    tok = pos_ref.shape[0]
    cap, d = back_ref.shape[1:]
    lane = lax.broadcasted_iota(jnp.int32, (tok, n), 1)
    pos = jnp.sum(jnp.where(lane == e, pos_ref[...], 0), axis=1, keepdims=True)
    gate = jnp.sum(jnp.where(lane == e, gate_ref[...], 0.0), axis=1, keepdims=True)
    sel = jnp.where(lax.broadcasted_iota(jnp.int32, (tok, cap), 1) == pos, 1.0, 0.0).astype(BF)

    @pl.when(e == 0)
    def _():
        acc[...] = jnp.zeros_like(acc)

    def cols(m, c):
        at = pl.ds(pl.multiple_of(m * 512, 512), 512)
        acc[:, at] += gate * dot(sel, back_ref[0, :, at])
        return c

    lax.fori_loop(0, d // 512, cols, 0)

    @pl.when(e == n - 1)
    def _():
        out_ref[...] = acc[...].astype(BF)


def combine(n, back, pos, gate):
    tok = pos.shape[0]
    cap, d = back.shape[0] // n, back.shape[1]
    return pl.pallas_call(
        functools.partial(combine_kernel, n),
        grid=(n,),
        in_specs=[pl.BlockSpec((1, cap, d), lambda e: (e, 0, 0)), pl.BlockSpec((tok, n), lambda e: (0, 0)), pl.BlockSpec((tok, n), lambda e: (0, 0))],
        out_specs=pl.BlockSpec((tok, d), lambda e: (0, 0)),
        out_shape=jax.ShapeDtypeStruct((tok, d), BF),
        scratch_shapes=[pltpu.VMEM((tok, d), F32)],
        compiler_params=pltpu.CompilerParams(dimension_semantics=("arbitrary",), vmem_limit_bytes=48 * 1024 * 1024),
        cost_estimate=pl.CostEstimate(flops=2 * n * tok * cap * d, bytes_accessed=back.size * 2 + tok * d * 2, transcendentals=0),
        name="combine",
    )(back.reshape(n, cap, d), pos, gate)


def solution(mesh):
    n_exp = mesh.shape["ep"]
    row_spec = P(("dp", "ep"), None)
    weight_spec = P("ep", None, None)
    grad_w_spec = P(("dp", "ep"), None, None)

    def local(x, route_idx, route_gate, w_gate, w_up, w_down, grad_y):
        tok = x.shape[0]
        cap = 3 * tok // 4
        meta = jnp.concatenate([route_idx.astype(F32), route_gate], axis=1).T
        own = route_idx[:, :, None] == jnp.arange(n_exp, dtype=jnp.int32)
        own_hit = jnp.any(own, axis=1)
        own_gate = jnp.sum(jnp.where(own, route_gate[:, :, None], 0.0), axis=1)
        own_pos = jnp.where(own_hit, jnp.cumsum(own_hit.astype(jnp.int32), axis=0) - 1, -1)

        rows, _, _, h, _, c, da, db, r, back_o, _, _, _ = layer(n_exp, cap, x, grad_y, meta, w_gate, w_up, w_down)
        back_r = lax.all_to_all(r, "ep", 0, 0, tiled=True)
        gwg = dot(rows, da, FIRST).astype(BF)
        gwu = dot(rows, db, FIRST).astype(BF)
        gwd = dot(h, c, FIRST).astype(BF)
        y = combine(n_exp, back_o, own_pos, own_gate)
        grad_x = combine(n_exp, back_r, own_pos, jnp.ones_like(own_gate))
        return y, grad_x, gwg[None], gwu[None], gwd[None]

    return jax.shard_map(local, mesh=mesh, in_specs=(row_spec, row_spec, row_spec, weight_spec, weight_spec, weight_spec, row_spec), out_specs=(row_spec, row_spec, grad_w_spec, grad_w_spec, grad_w_spec), check_vma=False)
```

```python
import functools

import jax
import jax.numpy as jnp
from jax import lax
from jax.experimental import pallas as pl
from jax.experimental.pallas import tpu as pltpu
from jax.sharding import PartitionSpec as P

MESH = pl.DeviceIdType.MESH
MID = (((1,), (0,)), ((), ()))
LAST = (((1,), (1,)), ((), ()))
FIRST = (((0,), (0,)), ((), ()))
BF = jnp.bfloat16
F32 = jnp.float32
FOLD_AT = 8


def dot(a, b, dims=MID):
    return lax.dot_general(a, b, dims, preferred_element_type=F32)


def iota(shape, dim):
    return lax.broadcasted_iota(jnp.int32, shape, dim)


def ones(mask):
    return jnp.where(mask, 1.0, 0.0)


def total(v, axis):
    return jnp.sum(v, axis=axis, keepdims=True)


def tile(t, size):
    return pl.ds(pl.multiple_of(t * size, size), size)


def layer_kernel(n, cap, x_ref, gy_ref, meta_ref, wg_ref, wu_ref, wd_ref,
                 y_out, gx_out, gwg_out, gwu_out, gwd_out, xr_out, a_out, b_out, h_out, o_out, c_out, da_out, db_out, r_out, back_o, back_r, fold_o, fold_r, sum_o, sum_r, part_o, part_r, xg, gyg, mg,
                 wg, wu, wd, xbuf, mbuf, tri, pbuf, posbuf, gatebuf, xr, ab_a, ab_b, hb, ob, cb, dab, dbb, acc, lay, cols_own, cols_far,
                 send_sem, recv_sem, give_sem, take_sem, wsem, lsem, outsem, vsem):
    tok, d = x_ref.shape
    ff = wd_ref.shape[1]
    half = tok // 2
    me = lax.axis_index("ep")
    chips = n // 2
    chip, core = me // 2, lax.rem(me, 2)
    right = lax.rem(chip + 1, chips) * 2 + core
    left = lax.rem(chip + chips - 1, chips) * 2 + core
    across = lax.rem(chip + 2, chips) * 2 + core
    mate = chip * 2 + 1 - core
    right_m = lax.rem(chip + 1, chips) * 2 + 1 - core
    left_m = lax.rem(chip + chips - 1, chips) * 2 + 1 - core
    across_m = lax.rem(chip + 2, chips) * 2 + 1 - core
    lean = lax.rem(1 - 2 * core + chips, chips)
    ahead = lax.rem(chip + lean, chips) * 2 + core
    behind = lax.rem(chip + chips - lean, chips) * 2 + core
    ahead_m = lax.rem(chip + lean, chips) * 2 + 1 - core
    behind_m = lax.rem(chip + chips - lean, chips) * 2 + 1 - core
    peers = (left, right, mate, left_m, right_m)

    barrier = pltpu.get_barrier_semaphore()
    for peer in peers:
        pl.semaphore_signal(barrier, inc=1, device_id={"ep": peer}, device_id_type=MESH)
    pl.semaphore_wait(barrier, len(peers))

    own = (x_ref, gy_ref, meta_ref)
    got = (xg, gyg, mg)

    def whole(item, slot):
        return got[item].at[slot]

    def part(item, slot, which):
        return got[item].at[slot, pl.ds(which * half, half)] if item < 2 else got[item].at[slot]

    def mine(item, which):
        return own[item].at[pl.ds(which * half, half)] if item == 1 else own[item]

    def leg(item, k):
        beside = part if item == 1 else lambda i, slot, which: got[i].at[slot]
        return (
            (mine(item, 0), beside(item, me, 0), right, beside(item, left, 0)),
            (mine(item, 0), beside(item, me, 0), left, beside(item, right, 0)),
            (own[item], whole(item, me), mate, whole(item, mate)),
            (part(item, left, 0), part(item, left, 0), right, part(item, across, 0)),
            (part(item, right, 1), part(item, right, 1), left, part(item, across, 1)),
            (whole(item, left), whole(item, left), mate, whole(item, left_m)),
            (whole(item, right), whole(item, right), mate, whole(item, right_m)),
            (whole(item, across), whole(item, across), mate, whole(item, across_m)),
            (mine(item, 1), part(item, me, 1), right, part(item, left, 1)),
            (mine(item, 1), part(item, me, 1), left, part(item, right, 1)),
        )[k]

    def remote(src, dst, out_sem, in_sem, peer):
        return pltpu.make_async_remote_copy(
            src_ref=src, dst_ref=dst, send_sem=out_sem, recv_sem=in_sem, device_id={"ep": peer}, device_id_type=MESH)

    def send(item, k):
        src, dst, peer, _ = leg(item, k)
        return remote(src, dst, send_sem.at[item, k], recv_sem.at[item, k], peer)

    def start(item, *ks):
        for k in ks:
            send(item, k).start()

    def land(item, *ks):
        for k in ks:
            ref = leg(item, k)[-1]
            remote(ref, ref, send_sem.at[item, k], recv_sem.at[item, k], mate).wait_recv()

    def rows_of(slot):
        return tile(slot, cap)

    made, back, fold = (o_out, r_out), (back_o, back_r), (fold_o, fold_r)
    sums, parts = (sum_o, sum_r), (part_o, part_r)
    piece = tok // 4
    routes = ((mate, mate), (behind, behind), (ahead_m, ahead_m), (behind_m, mate), (across, ahead), (across_m, behind_m))
    sources = (mate, ahead, ahead_m)

    def give(w, k):
        rows, peer = routes[k]
        dst = back[w].at[rows_of(me)] if k < 3 else fold[w].at[k - 3]
        return remote(made[w].at[rows_of(rows)], dst, give_sem.at[w, k], take_sem.at[w, k], peer)

    def give_sum(w, q):
        at = pl.ds(q * piece, piece)
        return remote(sums[w].at[at], parts[w].at[at], give_sem.at[w, 6 + q], take_sem.at[w, 6 + q], ahead)

    def take(w, k):
        ref = back[w].at[rows_of(sources[k])] if k < 3 else fold[w].at[k - 3] if k < 6 else parts[w].at[pl.ds((k - 6) * piece, piece)]
        remote(ref, ref, give_sem.at[w, k], take_sem.at[w, k], mate).wait_recv()

    start(2, 0, 1, 2)
    start(0, 0, 1, 2)
    start(1, 0, 1, 2)

    weights = [pltpu.make_async_copy(s.at[0], t, wsem.at[q]) for q, (s, t) in enumerate(((wg_ref, wg), (wu_ref, wu), (wd_ref, wd)))]
    for cp in weights:
        cp.start()
    for q in range(4):
        band = (tok // 4, tok)
        tri[tile(q, tok // 4), :] = ones(iota(band, 0) + q * (tok // 4) <= iota(band, 1)).astype(BF)
    for cp in weights:
        cp.wait()

    def is_forward(i):
        return (i < 2) | ((i >= 4) & (i < 10))

    def slot_of(i):
        j = jnp.where(i < 2, i, jnp.where(i < 10, i - 2, i - 8))
        hop = jnp.where(j < 2, 0, jnp.where(j >= 6, 2, jnp.where(lax.rem(j, 2) == 0, lean, chips - lean)))
        flip = (j == 1) | (j == 4) | (j == 5) | (j == 7)
        return j, lax.rem(chip + hop, chips) * 2 + jnp.where(flip, 1 - core, core)

    f_bufs = ((xr, xr_out), (ab_a, a_out), (ab_b, b_out), (hb, h_out), (ob, o_out))
    b_bufs = ((cb, c_out), (dab, da_out), (dbb, db_out), (ob, r_out))

    def out_copy(q, bufs, slot):
        src, dst = bufs[q]
        return pltpu.make_async_copy(src, dst.at[rows_of(slot)], outsem.at[q + (5 if bufs is b_bufs else 0)])

    wide = ff // 256
    rest = pl.ds(wide * 256, ff % 256)

    def loop(count, body):
        def run(t, c):
            body(t)
            return c

        lax.fori_loop(0, count, run, 0)

    def col_tiles(body):
        loop(wide, lambda t: body(tile(t, 256)))
        if ff % 256:
            body(rest)

    def model_tiles(body):
        loop(d // 512, lambda t: body(tile(t, 512)))

    def settle(i):
        last = i - 1

        @pl.when((i > 0) & is_forward(last))
        def _():
            for q in range(5):
                out_copy(q, f_bufs, 0).wait()

        @pl.when((i > 0) & jnp.logical_not(is_forward(last)))
        def _():
            for q in range(4):
                out_copy(q, b_bufs, 0).wait()

        for when, w, sends in (
            (2, 0, (0,)), (4, 1, (0,)), (7, 0, (1, 2)), (8, 0, (3,)), (9, 0, (4,)), (10, 0, (5,)),
            (12, 1, (1,)), (13, 1, (2,)), (14, 1, (3,)), (15, 1, (4,)), (16, 1, (5,))):
            @pl.when(i == when)
            def _(w=w, sends=sends):
                for k in sends:
                    give(w, k).start()

    def step(i):
        is_f = is_forward(i)
        j, slot = slot_of(i)

        def at(when):
            return pl.when(i == when)

        @at(1)
        def _():
            land(2, 2)
            land(0, 2)

        @at(3)
        def _():
            land(1, 2)
            land(2, 0, 1)
            land(0, 0, 1)
            start(2, 3, 5, 6)
            start(0, 3, 4, 5, 6)
            start(1, 8, 9)

        @at(6)
        def _():
            land(2, 5, 6)
            land(0, 5, 6)

        @at(8)
        def _():
            land(2, 3)
            land(0, 3, 4)
            start(2, 7)
            start(0, 7)
            land(1, 0, 1, 8, 9)
            start(1, 3, 4, 5, 6)

        @at(9)
        def _():
            land(2, 7)
            land(0, 7)

        @at(12)
        def _():
            land(1, 5, 6)

        @at(14)
        def _():
            land(1, 3, 4)
            start(1, 7)

        @at(15)
        def _():
            land(1, 7)

        def fetch(own_ref, got_ref, buf, sem):
            @pl.when(j == 0)
            def _():
                pltpu.make_async_copy(own_ref, buf, sem).start()

            @pl.when(j > 0)
            def _():
                pltpu.make_async_copy(got_ref.at[slot], buf, sem).start()

        def fetched(own_ref, buf, sem):
            pltpu.make_async_copy(own_ref, buf, sem).wait()

        def fill_p():
            pos = posbuf[j][0:1, :]
            for q in range(cap // 128):
                pbuf[tile(q, 128), :] = ones(iota((128, tok), 0) + q * 128 == pos).astype(BF)

        @pl.when(is_f)
        def _():
            fetch(meta_ref, mg, mbuf, lsem.at[1])
            fetch(x_ref, xg, xbuf, lsem.at[0])
            fetched(meta_ref, mbuf, lsem.at[1])
            sel = mbuf[0:4, :] == me.astype(F32)
            gatebuf[j] = jnp.broadcast_to(total(jnp.where(sel, mbuf[4:8, :], 0.0), 0), (8, tok))
            hit = total(ones(sel), 0)
            count = dot(jnp.broadcast_to(hit, (16, tok)).astype(BF), tri[:])[0:1, :]
            pos = jnp.where(hit > 0.0, count - 1.0, -1.0).astype(jnp.int32)
            posbuf[j] = jnp.broadcast_to(pos, (8, tok))
            fill_p()
            settle(i)
            fetched(x_ref, xbuf, lsem.at[0])

            def pick(cols):
                xr[:, cols] = dot(pbuf[:], xbuf[:, cols]).astype(BF)

            model_tiles(pick)
            out_copy(0, f_bufs, slot).start()

            def up(cols):
                a, b = dot(xr[:], wg[:, cols]), dot(xr[:], wu[:, cols])
                ab_a[:, cols] = a
                ab_b[:, cols] = b
                hb[:, cols] = (a * jax.nn.sigmoid(a) * b).astype(BF)

            col_tiles(up)
            for q in (1, 2, 3):
                out_copy(q, f_bufs, slot).start()

            def down(cols):
                ob[:, cols] = dot(hb[:], wd[:, cols]).astype(BF)

            model_tiles(down)

            @pl.when(j == 0)
            def _():
                pltpu.make_async_copy(ob, back_o.at[rows_of(me)], outsem.at[4]).start()

            @pl.when(j > 0)
            def _():
                out_copy(4, f_bufs, slot).start()

        @pl.when(jnp.logical_not(is_f))
        def _():
            fetch(gy_ref, gyg, xbuf, lsem.at[0])
            fill_p()
            settle(i)
            load_a = pltpu.make_async_copy(a_out.at[rows_of(slot)], ab_a, lsem.at[2])
            load_b = pltpu.make_async_copy(b_out.at[rows_of(slot)], ab_b, lsem.at[3])
            load_a.start()
            load_b.start()
            g = total(pbuf[:].astype(F32) * gatebuf[j][0:1, :], 1)
            fetched(gy_ref, xbuf, lsem.at[0])

            def pick(cols):
                cb[:, cols] = (g * dot(pbuf[:], xbuf[:, cols])).astype(BF)

            model_tiles(pick)
            out_copy(0, b_bufs, slot).start()
            load_a.wait()
            load_b.wait()

            def down_t(cols):
                dh = dot(cb[:], wd[cols, :], LAST).astype(BF).astype(F32)
                a, b = ab_a[:, cols], ab_b[:, cols]
                s = jax.nn.sigmoid(a)
                dab[:, cols] = (dh * b * (s * (1.0 + a * (1.0 - s)))).astype(BF)
                dbb[:, cols] = (dh * (a * s)).astype(BF)

            col_tiles(down_t)
            out_copy(1, b_bufs, slot).start()
            out_copy(2, b_bufs, slot).start()

            def up_t(cols):
                ob[:, cols] = (dot(dab[:], wg[cols, :], LAST) + dot(dbb[:], wu[cols, :], LAST)).astype(BF)

            model_tiles(up_t)

            @pl.when(j == 0)
            def _():
                pltpu.make_async_copy(ob, back_r.at[rows_of(me)], outsem.at[8]).start()

            @pl.when(j > 0)
            def _():
                out_copy(3, b_bufs, slot).start()

    loop(2 * n, step)
    settle(2 * n)

    def lay_out(meta_src, cols):
        cp = pltpu.make_async_copy(meta_src, mbuf, lsem.at[1])
        cp.start()
        cp.wait()
        which = iota((n, tok), 0).astype(F32)
        hit, gate = jnp.zeros((n, tok), F32), jnp.zeros((n, tok), F32)
        for k in range(4):
            match = mbuf[k:k + 1, :] == which
            hit = hit + ones(match)
            gate = gate + jnp.where(match, mbuf[4 + k:5 + k, :], 0.0)
        count = dot(jnp.concatenate([hit, hit], axis=0).astype(BF), tri[:])[0:n, :]
        lay[:] = jnp.zeros_like(lay)
        lay[0:n, :] = jnp.where(hit > 0.0, count - 1.0, -1.0)
        lay[n:2 * n, :] = gate
        cols[:] = lay[:].T

    lay_out(meta_ref, cols_own)
    lay_out(mg.at[ahead], cols_far)
    picked = xbuf.at[:, pl.ds(0, cap)]

    def gains(w, cols, experts, srcs, waits):
        acc[:] = jnp.zeros_like(acc)

        def gain(q):
            e = experts[0]
            for k in range(4):
                e = jnp.where(q == k, experts[k], e)

                @pl.when(q == k)
                def _(k=k):
                    if waits[k] is not None:
                        take(w, waits[k])
                    pltpu.make_async_copy(srcs[k], cb, lsem.at[0]).start()

            lane = iota((tok, 128), 1)

            def column(k):
                return total(jnp.where(lane == k, cols[:], 0.0), 1)

            picked[:] = ones(iota((tok, cap), 1) == column(e).astype(jnp.int32)).astype(BF)
            gate = column(e + n) if w == 0 else 1.0
            pltpu.make_async_copy(srcs[0], cb, lsem.at[0]).wait()

            def add(at):
                part = dot(picked[:], cb[:, at])
                acc[:, at] += gate * part

            model_tiles(add)

        loop(4, gain)

    def fold_up(w):
        gains(w, cols_far, (me, mate, behind, behind_m),
              (made[w].at[rows_of(ahead)], fold[w].at[0], fold[w].at[1], fold[w].at[2]), (None, 3, 4, 5))
        cp = pltpu.make_async_copy(acc, sums[w], lsem.at[1])
        cp.start()
        cp.wait()
        for q in range(4):
            give_sum(w, q).start()

    def finish(w, out):
        gains(w, cols_own, (me, mate, ahead, ahead_m),
              tuple(back[w].at[rows_of(e)] for e in (me, mate, ahead, ahead_m)), (None, 0, 1, 2))
        stores = []
        for q in range(4):
            at = pl.ds(q * piece, piece)
            take(w, 6 + q)
            halves = ((ab_a, 0), (ab_b, d // 2))
            loads = [pltpu.make_async_copy(parts[w].at[at, pl.ds(c0, d // 2)], b.at[pl.ds(0, piece), pl.ds(0, d // 2)], vsem.at[2 + k])
                     for k, (b, c0) in enumerate(halves)]
            for cp in loads:
                cp.start()
            for cp in loads:
                cp.wait()
            for b, c0 in halves:
                cols = pl.ds(c0, d // 2)
                xbuf[at, cols] = (acc[at, cols] + b[pl.ds(0, piece), pl.ds(0, d // 2)]).astype(BF)
            stores.append(pltpu.make_async_copy(xbuf.at[at], out.at[at], outsem.at[3 + q]))
            stores[-1].start()
        for cp in stores:
            cp.wait()

    fold_up(0)

    for f0, fn in ((0, cap), (cap, ff - cap)):
        d_bufs = ((hb.at[:, pl.ds(0, fn)], cb), (dab.at[:, pl.ds(0, fn)], xr))
        h_turned = ob.at[pl.ds(0, fn), pl.ds(0, cap)]
        stage_d = xbuf.at[pl.ds(0, fn), :]

        def d_load(blk, p, f0=f0, fn=fn, d_bufs=d_bufs):
            srcs = (h_out.at[rows_of(blk), pl.ds(f0, fn)], c_out.at[rows_of(blk)])
            return [pltpu.make_async_copy(a, b, vsem.at[p * 3 + q]) for q, (a, b) in enumerate(zip(srcs, d_bufs[p]))]

        def d_step(blk, p, fn=fn, d_bufs=d_bufs, h_turned=h_turned, d_load=d_load):
            @pl.when(blk + 1 < n)
            def _():
                for cp in d_load(blk + 1, 1 - p):
                    cp.start()

            for cp in d_load(blk, p):
                cp.wait()
            h_turned[:] = d_bufs[p][0][:].T

            @pl.when(blk == 0)
            def _():
                acc[pl.ds(0, fn), :] = jnp.zeros((fn, d), F32)

            def add(cols):
                acc[pl.ds(0, fn), cols] += dot(h_turned[:], d_bufs[p][1][:, cols])

            model_tiles(add)

        def d_pair(u, d_step=d_step):
            d_step(2 * u, 0)
            d_step(2 * u + 1, 1)

        for cp in d_load(0, 0):
            cp.start()
        loop(n // 2, d_pair)
        stage_d[:] = acc[pl.ds(0, fn), :].astype(BF)
        store = pltpu.make_async_copy(stage_d, gwd_out.at[0, pl.ds(f0, fn)], outsem.at[2])
        store.start()
        store.wait()

    band = 512
    gu_bufs = ((pbuf.at[:, pl.ds(0, band)], dab, dbb), (pbuf.at[:, pl.ds(band, band)], hb, xbuf.at[pl.ds(0, cap), pl.ds(0, ff)]))
    stage_g, stage_u = ob.at[pl.ds(0, band), pl.ds(0, ff)], xr.at[pl.ds(0, band), pl.ds(0, ff)]
    turned = cb.at[pl.ds(0, band), pl.ds(0, cap)]

    def gu_load(t, p):
        m, blk = t // n, lax.rem(t, n)
        srcs = (xr_out.at[rows_of(blk), pl.ds(pl.multiple_of(m * band, band), band)], da_out.at[rows_of(blk)], db_out.at[rows_of(blk)])
        return [pltpu.make_async_copy(a, b, vsem.at[p * 3 + q]) for q, (a, b) in enumerate(zip(srcs, gu_bufs[p]))]

    def gu_store(m):
        at = pl.ds(pl.multiple_of(m * band, band), band)
        return [pltpu.make_async_copy(stage_g, gwg_out.at[0, at], outsem.at[0]), pltpu.make_async_copy(stage_u, gwu_out.at[0, at], outsem.at[1])]

    def gu_step(t, p):
        @pl.when(t + 1 < (d // band) * n)
        def _():
            for cp in gu_load(t + 1, 1 - p):
                cp.start()

        for cp in gu_load(t, p):
            cp.wait()
        xt, g_blk, u_blk = gu_bufs[p]
        turned[:] = xt[:].T

        @pl.when(lax.rem(t, n) == 0)
        def _():
            acc[:, pl.ds(0, ff)] = jnp.zeros((2 * band, ff), F32)

        def add(cols):
            acc[pl.ds(0, band), cols] += dot(turned[:], g_blk[:, cols])
            acc[pl.ds(band, band), cols] += dot(turned[:], u_blk[:, cols])

        col_tiles(add)

    def gu_pair(u):
        @pl.when(u == FOLD_AT)
        def _():
            fold_up(1)

        gu_step(2 * u, 0)
        gu_step(2 * u + 1, 1)
        m = (2 * u + 1) // n

        @pl.when(lax.rem(2 * u + 1, n) == n - 1)
        def _():
            @pl.when(m > 0)
            def _():
                for cp in gu_store(0):
                    cp.wait()

            stage_g[:] = acc[pl.ds(0, band), pl.ds(0, ff)].astype(BF)
            stage_u[:] = acc[pl.ds(band, band), pl.ds(0, ff)].astype(BF)
            for cp in gu_store(m):
                cp.start()

    for cp in gu_load(0, 0):
        cp.start()
    loop((d // band) * n // 2, gu_pair)
    for cp in gu_store(0):
        cp.wait()

    finish(0, y_out)
    finish(1, gx_out)
    for w in range(2):
        for k in range(len(routes)):
            give(w, k).wait_send()
        for q in range(4):
            give_sum(w, q).wait_send()
    for item, ks in enumerate((range(8), range(10), (0, 1, 2, 3, 5, 6, 7))):
        for k in ks:
            send(item, k).wait_send()


def layer(n, cap, x, gy, meta, w_gate, w_up, w_down):
    tok, d = x.shape
    ff = w_down.shape[1]
    rows = n * cap
    hbm = pl.BlockSpec(memory_space=pltpu.HBM)
    shapes = [
        ((tok, d), BF), ((tok, d), BF), ((1, d, ff), BF), ((1, d, ff), BF), ((1, ff, d), BF),
        ((rows, d), BF), ((rows, ff), F32), ((rows, ff), F32), ((rows, ff), BF), ((rows, d), BF), ((rows, d), BF),
        ((rows, ff), BF), ((rows, ff), BF), ((rows, d), BF), ((rows, d), BF), ((rows, d), BF),
        ((3, cap, d), BF), ((3, cap, d), BF), ((tok, d), F32), ((tok, d), F32), ((tok, d), F32), ((tok, d), F32),
        ((n, tok, d), BF), ((n, tok, d), BF), ((n, 8, tok), F32)]
    dma = pltpu.SemaphoreType.DMA
    return pl.pallas_call(
        functools.partial(layer_kernel, n, cap),
        out_shape=[jax.ShapeDtypeStruct(s, t) for s, t in shapes],
        in_specs=[hbm] * 6,
        out_specs=[hbm] * len(shapes),
        scratch_shapes=[
            pltpu.VMEM((d, ff), BF),
            pltpu.VMEM((d, ff), BF),
            pltpu.VMEM((ff, d), BF),
            pltpu.VMEM((tok, d), BF),
            pltpu.VMEM((8, tok), F32),
            pltpu.VMEM((tok, tok), BF),
            pltpu.VMEM((cap, tok), BF),
            pltpu.VMEM((n, 8, tok), jnp.int32),
            pltpu.VMEM((n, 8, tok), F32),
            pltpu.VMEM((cap, d), BF),
            pltpu.VMEM((cap, ff), F32),
            pltpu.VMEM((cap, ff), F32),
            pltpu.VMEM((cap, ff), BF),
            pltpu.VMEM((cap, d), BF),
            pltpu.VMEM((cap, d), BF),
            pltpu.VMEM((cap, ff), BF),
            pltpu.VMEM((cap, ff), BF),
            pltpu.VMEM((tok, d), F32),
            pltpu.VMEM((128, tok), F32),
            pltpu.VMEM((tok, 128), F32),
            pltpu.VMEM((tok, 128), F32),
            dma((3, 10)), dma((3, 10)), dma((2, 10)), dma((2, 10)), dma((3,)), dma((4,)), dma((9,)), dma((6,)),
        ],
        compiler_params=pltpu.CompilerParams(collective_id=0, has_side_effects=True, vmem_limit_bytes=67043328),
        cost_estimate=pl.CostEstimate(flops=2 * rows * d * (6 * ff + 2 * tok), bytes_accessed=700 * 1024 * 1024, transcendentals=2 * rows * ff),
        name="layer",
    )(x, gy, meta, w_gate, w_up, w_down)


def solution(mesh):
    n_exp = mesh.shape["ep"]
    row_spec = P(("dp", "ep"), None)
    weight_spec = P("ep", None, None)
    grad_w_spec = P(("dp", "ep"), None, None)

    def local(x, route_idx, route_gate, w_gate, w_up, w_down, grad_y):
        tok = x.shape[0]
        cap = 3 * tok // 4
        meta = jnp.concatenate([route_idx.astype(F32), route_gate], axis=1).T
        return tuple(layer(n_exp, cap, x, grad_y, meta, w_gate, w_up, w_down)[:5])

    return jax.shard_map(local, mesh=mesh, in_specs=(row_spec, row_spec, row_spec, weight_spec, weight_spec, weight_spec, row_spec), out_specs=(row_spec, row_spec, grad_w_spec, grad_w_spec, grad_w_spec), check_vma=False)
```
